32 devices in a mesh: bias: 2 (over x), ea: 16 (over z, y, core).
Axes of the slice: x: 2, y: 2, z: 4, core: 2. Of those that a mesh axis runs over, the one named last changes fastest.
Arguments:
- g_lesser: bfloat16 [512, 2, 256, 256], P(('bias', 'ea')), parts along dimension 0, may hold values from -6 to 6
- g_greater: bfloat16 [512, 2, 256, 256], P(('bias', 'ea')), parts along dimension 0, may hold values from -6 to 6
- g_free: bfloat16 [512, 2, 256, 256], P(('bias', 'ea')), parts along dimension 0, may hold values from -3 to 3
- coulomb: bfloat16 [256, 256], replicated, may hold values from -0.375 to 0.375
Outputs:
- g_new: bfloat16 [512, 2, 256, 256], P(('bias', 'ea')), parts along dimension 0
The draws below stay inside these ranges and needn't reach their ends.
There are 2 independent parts, one for each index of `bias`. The reference program is written for one: setup_inputs(seed, part) draws one part's arguments, and reference() takes and returns one part's arrays. A program takes and returns all parts, laid end to end along the dimension named above; an argument that names none is the same for every part. Nothing has to cross between parts.
All inputs are finite; a program needn't handle non-finite values.
Results may differ from the reference program's by a relative error of at most 0.022.
Values may be sent and summed in bfloat16 or wider, within the bound.
A program may use at most 192 MiB of HBM per device.

```python
import jax
import jax.numpy as jnp

NO = 256
NE = 256


def levels(rng, extent, shards, least, top_value):
    def one(position, parts):
        steps = jax.random.uniform(jax.random.fold_in(jax.random.fold_in(rng, 6), position), (parts,), jnp.float32, least / len(shards), top_value / len(shards))
        return jnp.repeat(jnp.exp(steps), extent[position] // parts).reshape((-1,) + (1,) * (len(extent) - position - 1))

    gain = one(*shards[0])
    for cut in shards[1:]:
        gain = gain * one(*cut)
    return gain


def gaussian(own_key, shape, width, reach, split=(), held_as=jnp.bfloat16):
    level = levels(own_key, shape, split, -0.22, 0.18) if split else 1.0
    entries = jax.random.normal(own_key, shape, jnp.float32) * width * level
    return jnp.minimum(jnp.maximum(entries, -reach), reach).astype(held_as)


def setup_inputs(seed: int = 0, part: int = 0) -> dict:
    key_list = jax.random.split(jax.random.key(seed), 5)
    part_keys = jax.random.split(jax.random.fold_in(key_list[4], part), 5)
    g_lesser = gaussian(part_keys[0], (NE, 2, NO, NO), 1.0, 6.0, ((0, 16),))
    g_greater = gaussian(part_keys[1], (NE, 2, NO, NO), 1.0, 6.0, ((0, 16),))
    g_free = gaussian(part_keys[2], (NE, 2, NO, NO), 0.5, 3.0, ((0, 16),))
    coulomb = gaussian(key_list[3], (NO, NO), NO ** -0.5, 0.375)
    return dict(g_lesser=g_lesser, g_greater=g_greater, g_free=g_free, coulomb=coulomb)


def as_complex(block):
    return block[:, 0].astype(jnp.float32) + 1j * block[:, 1].astype(jnp.float32)


def batched(left, right):
    return jnp.einsum("eij,ejk->eik", left.astype(jnp.float32), right.astype(jnp.float32))


def reference(g_lesser, g_greater, g_free, coulomb):
    length = 2 * NE
    lesser = as_complex(g_lesser)
    greater_t = jnp.swapaxes(as_complex(g_greater), 1, 2)
    spec_lesser = jnp.fft.fft(lesser, n=length, axis=0)
    spec_greater = jnp.fft.ifft(greater_t, n=length, axis=0) * length
    polar = jnp.fft.ifft(spec_lesser * spec_greater, axis=0)[:NE] / NE
    polar_real = polar.real.astype(jnp.bfloat16)
    polar_imag = polar.imag.astype(jnp.bfloat16)
    volts = coulomb.astype(jnp.float32)
    mixed_real = jnp.einsum("eij,jk->eik", polar_real.astype(jnp.float32), volts).astype(jnp.bfloat16)
    mixed_imag = jnp.einsum("eij,jk->eik", polar_imag.astype(jnp.float32), volts).astype(jnp.bfloat16)
    square_real = batched(mixed_real, mixed_real) - batched(mixed_imag, mixed_imag)
    square_imag = batched(mixed_real, mixed_imag) + batched(mixed_imag, mixed_real)
    inner_real = (mixed_real.astype(jnp.float32) + square_real).astype(jnp.bfloat16)
    inner_imag = (mixed_imag.astype(jnp.float32) + square_imag).astype(jnp.bfloat16)
    screen_real = (volts[None] + jnp.einsum("ij,ejk->eik", volts, inner_real.astype(jnp.float32))).astype(jnp.bfloat16)
    screen_imag = jnp.einsum("ij,ejk->eik", volts, inner_imag.astype(jnp.float32)).astype(jnp.bfloat16)
    screen = screen_real.astype(jnp.float32) + 1j * screen_imag.astype(jnp.float32)
    spec_screen = jnp.fft.fft(screen, n=length, axis=0)
    sigma = jnp.fft.ifft(spec_lesser * spec_screen, axis=0)[:NE] / NE
    sigma_real = sigma.real.astype(jnp.bfloat16)
    sigma_imag = sigma.imag.astype(jnp.bfloat16)
    free_real = g_free[:, 0]
    free_imag = g_free[:, 1]
    right_real = (batched(sigma_real, free_real) - batched(sigma_imag, free_imag)).astype(jnp.bfloat16)
    right_imag = (batched(sigma_real, free_imag) + batched(sigma_imag, free_real)).astype(jnp.bfloat16)
    out_real = free_real.astype(jnp.float32) + batched(free_real, right_real) - batched(free_imag, right_imag)
    out_imag = free_imag.astype(jnp.float32) + batched(free_real, right_imag) + batched(free_imag, right_real)
    return jnp.stack([out_real, out_imag], axis=1).astype(jnp.bfloat16)
```

```python
import functools
import math

import jax
import jax.numpy as jnp
import numpy as np
from jax import lax
from jax.experimental import pallas as pl
from jax.experimental.pallas import tpu as pltpu
from jax.sharding import PartitionSpec as P

NE = 256


def dft_tables(length, count):
    freq = jnp.arange(length, dtype=jnp.int32)
    places = jnp.arange(count, dtype=jnp.int32)
    phase = freq[:, None] * places[None, :] % length
    angle = phase.astype(jnp.float32) * (2.0 * math.pi / length)
    cosine = jnp.cos(angle)
    sine = jnp.sin(angle)
    stacked = jnp.concatenate([cosine, sine], axis=0)
    upper = stacked.astype(jnp.bfloat16)
    lower = (stacked - upper.astype(jnp.float32)).astype(jnp.bfloat16)
    backward = jnp.concatenate([cosine.T, sine.T], axis=0)
    return (upper, lower, backward)


def forward(tables, block, sign):
    upper, lower = tables
    length = upper.shape[0] // 2
    real_part = block[:, 0].reshape(block.shape[0], -1)
    imag_part = block[:, 1].reshape(block.shape[0], -1)
    width = real_part.shape[1]
    joined = jnp.concatenate([real_part, imag_part], axis=1)
    result = jnp.dot(upper, joined, preferred_element_type=jnp.float32)
    result = result + jnp.dot(lower, joined, preferred_element_type=jnp.float32)
    cos_real = result[:length, :width]
    cos_imag = result[:length, width:]
    sin_real = result[length:, :width]
    sin_imag = result[length:, width:]
    return (cos_real - sign * sin_imag, cos_imag + sign * sin_real)


def inverse(backward, real_part, imag_part, scale):
    count = backward.shape[0] // 2
    width = real_part.shape[1]
    joined = jnp.concatenate([real_part, imag_part], axis=1)
    result = jnp.dot(
        backward, joined, precision=lax.Precision.HIGH, preferred_element_type=jnp.float32
    )
    cos_real = result[:count, :width]
    cos_imag = result[:count, width:]
    sin_real = result[count:, :width]
    sin_imag = result[count:, width:]
    return ((cos_real - sin_imag) * scale, (cos_imag + sin_real) * scale)


def complex_mul(left, right):
    return (left[0] * right[0] - left[1] * right[1], left[0] * right[1] + left[1] * right[0])


def restack(real_part, imag_part, shape):
    return jnp.stack([real_part.reshape(shape), imag_part.reshape(shape)], axis=1).astype(
        jnp.bfloat16
    )


def batched(left, right):
    return jnp.einsum("eij,ejk->eik", left, right, preferred_element_type=jnp.float32)


def dyson(sigma_real, sigma_imag, g_free):
    free_real = g_free[:, 0]
    free_imag = g_free[:, 1]
    right_real = (batched(sigma_real, free_real) - batched(sigma_imag, free_imag)).astype(
        jnp.bfloat16
    )
    right_imag = (batched(sigma_real, free_imag) + batched(sigma_imag, free_real)).astype(
        jnp.bfloat16
    )
    out_real = (
        free_real.astype(jnp.float32)
        + batched(free_real, right_real)
        - batched(free_imag, right_imag)
    )
    out_imag = (
        free_imag.astype(jnp.float32)
        + batched(free_real, right_imag)
        + batched(free_imag, right_real)
    )
    return jnp.stack([out_real, out_imag], axis=1).astype(jnp.bfloat16)


def plain(g_lesser, g_greater, g_free, coulomb):
    length = 2 * NE
    upper, lower, backward = dft_tables(length, NE)
    tables = (upper, lower)
    scale = 1.0 / (length * NE)
    greater_t = jnp.swapaxes(g_greater, 2, 3)
    lesser_rows, greater_rows = (
        lax.all_to_all(g_lesser, "ea", split_axis=2, concat_axis=0, tiled=True),
        lax.all_to_all(greater_t, "ea", split_axis=2, concat_axis=0, tiled=True),
    )
    spec_lesser = forward(tables, lesser_rows, -1.0)
    element_shape = (NE, lesser_rows.shape[2], lesser_rows.shape[3])
    spec_greater = forward(tables, greater_rows, 1.0)
    joined = complex_mul(spec_lesser, spec_greater)
    polar_real, polar_imag = inverse(backward, joined[0], joined[1], scale)
    polar_rows = restack(polar_real, polar_imag, element_shape)
    polar = lax.all_to_all(polar_rows, "ea", split_axis=0, concat_axis=2, tiled=True)
    mixed_real = jnp.einsum(
        "eij,jk->eik", polar[:, 0], coulomb, preferred_element_type=jnp.float32
    ).astype(jnp.bfloat16)
    mixed_imag = jnp.einsum(
        "eij,jk->eik", polar[:, 1], coulomb, preferred_element_type=jnp.float32
    ).astype(jnp.bfloat16)
    square_real = batched(mixed_real, mixed_real) - batched(mixed_imag, mixed_imag)
    square_imag = batched(mixed_real, mixed_imag) + batched(mixed_imag, mixed_real)
    inner_real = (mixed_real.astype(jnp.float32) + square_real).astype(jnp.bfloat16)
    inner_imag = (mixed_imag.astype(jnp.float32) + square_imag).astype(jnp.bfloat16)
    screen_real = coulomb.astype(jnp.float32)[None] + jnp.einsum(
        "ij,ejk->eik", coulomb, inner_real, preferred_element_type=jnp.float32
    )
    screen_imag = jnp.einsum("ij,ejk->eik", coulomb, inner_imag, preferred_element_type=jnp.float32)
    screen = jnp.stack([screen_real, screen_imag], axis=1).astype(jnp.bfloat16)
    screen_rows = lax.all_to_all(screen, "ea", split_axis=2, concat_axis=0, tiled=True)
    spec_screen = forward(tables, screen_rows, -1.0)
    folded = complex_mul(spec_lesser, spec_screen)
    sigma_real, sigma_imag = inverse(backward, folded[0], folded[1], scale)
    sigma_rows = restack(sigma_real, sigma_imag, element_shape)
    sigma = lax.all_to_all(sigma_rows, "ea", split_axis=0, concat_axis=2, tiled=True)
    return dyson(sigma[:, 0], sigma[:, 1], g_free)


MESH = pl.DeviceIdType.MESH
CHUNKS = 4
VMEM_BYTES = 60 * 1024 * 1024


def transform_table(count):
    length = 2 * count
    phase = np.arange(length)[:, None] * np.arange(count)[None, :] % length
    angle = phase * (2.0 * math.pi / length)
    cosine, sine = np.cos(angle), np.sin(angle)
    return np.block([[cosine, sine], [-sine, cosine]]).astype(np.float32)


def greet(n):
    me = lax.axis_index("ea")
    barrier = pltpu.get_barrier_semaphore()

    def hello(k, carry):
        pl.semaphore_signal(
            barrier, inc=1, device_id={"ea": lax.rem(me + k, n)}, device_id_type=MESH
        )
        return carry

    lax.fori_loop(1, n, hello, 0)
    pl.semaphore_wait(barrier, n - 1)


def exchange_kernel(
    n, count, first, scale, *refs
):
    if first:
        (lesser, other, table, table_t, volts, out, kept,
         lesser_buf, other_buf, folded, in_send, in_recv, out_send, out_recv, own_in, own_out, keep) = refs
        streams = ((lesser, lesser_buf), (other, other_buf))
    else:
        (kept, other, table, table_t, out,
         lesser_buf, other_buf, folded, in_send, in_recv, out_send, out_recv, own_in, own_out, keep) = refs
        streams = ((other, other_buf),)
    me = lax.axis_index("ea")
    rows = folded.shape[1]
    each = count // n
    group = rows // CHUNKS

    def incoming(s, q, k):
        peer = lax.rem(me + k, n)
        source, target = streams[s]
        return pltpu.make_async_remote_copy(
            src_ref=source.at[:, pl.ds(peer * rows + q * group, group)],
            dst_ref=target.at[:, pl.ds(q * group, group), pl.ds(me * each, each)],
            send_sem=in_send.at[s, q, k],
            recv_sem=in_recv.at[s, q, k],
            device_id={"ea": peer},
            device_id_type=MESH,
        )

    def outgoing(q, k):
        peer = lax.rem(me + k, n)
        return pltpu.make_async_remote_copy(
            src_ref=folded.at[:, pl.ds(q * group, group), pl.ds(peer * each, each)],
            dst_ref=out.at[:, pl.ds(me * rows + q * group, group)],
            send_sem=out_send.at[q, k],
            recv_sem=out_recv.at[q, k],
            device_id={"ea": peer},
            device_id_type=MESH,
        )

    def own_incoming(s):
        source, target = streams[s]
        return pltpu.make_async_copy(
            source.at[:, pl.ds(me * rows, rows)],
            target.at[:, :, pl.ds(me * each, each)],
            own_in.at[s],
        )

    if not first:
        pltpu.make_async_copy(kept, lesser_buf, keep).start()
    for s in range(len(streams)):
        own_incoming(s).start()
    greet(n)

    def send_chunk(q, carry):
        for s in range(len(streams)):
            def send_one(k, inner):
                incoming(s, q, k).start()
                return inner
            lax.fori_loop(1, n, send_one, 0)
        return carry

    lax.fori_loop(0, CHUNKS, send_chunk, 0)
    for s in range(len(streams)):
        own_incoming(s).wait()
    if not first:
        pltpu.make_async_copy(kept, lesser_buf, keep).wait()

    length = 2 * count

    def fold(row, carry):
        left = jnp.concatenate([lesser_buf[0, row], lesser_buf[1, row]], axis=0)
        imag = other_buf[1, row]
        right = jnp.concatenate([other_buf[0, row], -imag if first else imag], axis=0)
        left_spec = jnp.dot(table[...], left, preferred_element_type=jnp.float32)
        right_spec = jnp.dot(table[...], right, preferred_element_type=jnp.float32)
        left_real, left_imag = left_spec[:length], left_spec[length:]
        right_real, right_imag = right_spec[:length], right_spec[length:]
        if first:
            real = left_real * right_real + left_imag * right_imag
            imag = left_imag * right_real - left_real * right_imag
        else:
            real = left_real * right_real - left_imag * right_imag
            imag = left_real * right_imag + left_imag * right_real
        product = jnp.concatenate([real, imag], axis=0).astype(jnp.bfloat16)
        result = jnp.dot(table_t[...], product, preferred_element_type=jnp.float32) * scale
        result = result.astype(jnp.bfloat16)
        if first:
            result = jnp.dot(result, volts[...], preferred_element_type=jnp.float32)
            result = result.astype(jnp.bfloat16)
        folded[0, row] = result[:count]
        folded[1, row] = result[count:]
        return carry

    def work(q, carry):
        for s in range(len(streams)):
            def wait_one(k, inner):
                incoming(s, q, k).wait()
                return inner
            lax.fori_loop(1, n, wait_one, 0)
        lax.fori_loop(q * group, (q + 1) * group, fold, 0)

        def send_one(k, inner):
            outgoing(q, k).start()
            return inner

        lax.fori_loop(1, n, send_one, 0)
        return carry

    lax.fori_loop(0, CHUNKS, work, 0)
    own_result = pltpu.make_async_copy(
        folded.at[:, :, pl.ds(me * each, each)], out.at[:, pl.ds(me * rows, rows)], own_out
    )
    own_result.start()
    if first:
        keeping = pltpu.make_async_copy(lesser_buf, kept, keep)
        keeping.start()

    def finish(q, carry):
        def wait_one(k, inner):
            outgoing(q, k).wait()
            return inner
        return lax.fori_loop(1, n, wait_one, carry)

    lax.fori_loop(0, CHUNKS, finish, 0)
    own_result.wait()
    if first:
        keeping.wait()


def exchange(n, count, first, scale, operands):
    two, orbitals, each, width = operands[1].shape
    rows = orbitals // n
    hbm = pl.BlockSpec(memory_space=pl.ANY)
    vmem = pl.BlockSpec(memory_space=pltpu.VMEM)
    streams = 2 if first else 1
    out_shape = [jax.ShapeDtypeStruct((2, orbitals, each, width), jnp.bfloat16)]
    if first:
        out_shape.append(jax.ShapeDtypeStruct((2, rows, count, width), jnp.bfloat16))
    buffer = pltpu.VMEM((2, rows, count, width), jnp.bfloat16)
    dma = pltpu.SemaphoreType.DMA
    return pl.pallas_call(
        functools.partial(exchange_kernel, n, count, first, scale),
        name="polarize" if first else "dress",
        out_shape=out_shape,
        in_specs=[hbm, hbm] + [vmem] * (len(operands) - 2),
        out_specs=[hbm] * len(out_shape),
        scratch_shapes=[
            buffer, buffer, buffer,
            dma((streams, CHUNKS, n)), dma((streams, CHUNKS, n)),
            dma((CHUNKS, n)), dma((CHUNKS, n)),
            dma((streams,)), dma, dma,
        ],
        compiler_params=pltpu.CompilerParams(
            collective_id=0 if first else 1, has_side_effects=True, vmem_limit_bytes=VMEM_BYTES
        ),
    )(*operands)


def per_device(n, g_lesser, g_greater, g_free, coulomb):
    each, _, orbitals, _ = g_lesser.shape
    count = n * each
    if each % 16 or orbitals % (n * CHUNKS):
        return plain(g_lesser, g_greater, g_free, coulomb)
    scale = 1.0 / (2 * count * count)
    full = transform_table(count)
    table = jnp.asarray(full).astype(jnp.bfloat16)
    table_t = jnp.asarray(full.T).astype(jnp.bfloat16)
    lesser = jnp.transpose(g_lesser, (1, 2, 0, 3))
    greater = jnp.transpose(g_greater, (1, 3, 0, 2))
    mixed, kept = exchange(n, count, True, scale, (lesser, greater, table, table_t, coulomb))
    mixed = jnp.transpose(mixed, (0, 2, 1, 3))
    mixed_real, mixed_imag = mixed[0], mixed[1]
    square_real = batched(mixed_real, mixed_real) - batched(mixed_imag, mixed_imag)
    square_imag = batched(mixed_real, mixed_imag) + batched(mixed_imag, mixed_real)
    inner_real = (mixed_real.astype(jnp.float32) + square_real).astype(jnp.bfloat16)
    inner_imag = (mixed_imag.astype(jnp.float32) + square_imag).astype(jnp.bfloat16)
    screen_real = coulomb.astype(jnp.float32)[:, None] + jnp.einsum(
        "ij,ejk->iek", coulomb, inner_real, preferred_element_type=jnp.float32
    )
    screen_imag = jnp.einsum("ij,ejk->iek", coulomb, inner_imag, preferred_element_type=jnp.float32)
    screen = jnp.stack([screen_real.astype(jnp.bfloat16), screen_imag.astype(jnp.bfloat16)], axis=0)
    (sigma,) = exchange(n, count, False, scale, (kept, screen, table, table_t))
    sigma = jnp.transpose(sigma, (0, 2, 1, 3))
    return dyson(sigma[0], sigma[1], g_free)


def solution(mesh):
    return jax.shard_map(
        functools.partial(per_device, mesh.shape["ea"]),
        mesh=mesh,
        in_specs=(
            P(("bias", "ea"), None, None, None),
            P(("bias", "ea"), None, None, None),
            P(("bias", "ea"), None, None, None),
            P(),
        ),
        out_specs=P(("bias", "ea"), None, None, None),
        check_vma=False,
    )
```

```python
import functools
import math

import jax
import jax.numpy as jnp
import numpy as np
from jax import lax
from jax.experimental import pallas as pl
from jax.experimental.pallas import tpu as pltpu
from jax.sharding import PartitionSpec as P

NE = 256


def dft_tables(length, count):
    freq = jnp.arange(length, dtype=jnp.int32)
    places = jnp.arange(count, dtype=jnp.int32)
    phase = freq[:, None] * places[None, :] % length
    angle = phase.astype(jnp.float32) * (2.0 * math.pi / length)
    cosine = jnp.cos(angle)
    sine = jnp.sin(angle)
    stacked = jnp.concatenate([cosine, sine], axis=0)
    upper = stacked.astype(jnp.bfloat16)
    lower = (stacked - upper.astype(jnp.float32)).astype(jnp.bfloat16)
    backward = jnp.concatenate([cosine.T, sine.T], axis=0)
    return (upper, lower, backward)


def forward(tables, block, sign):
    upper, lower = tables
    length = upper.shape[0] // 2
    real_part = block[:, 0].reshape(block.shape[0], -1)
    imag_part = block[:, 1].reshape(block.shape[0], -1)
    width = real_part.shape[1]
    joined = jnp.concatenate([real_part, imag_part], axis=1)
    result = jnp.dot(upper, joined, preferred_element_type=jnp.float32)
    result = result + jnp.dot(lower, joined, preferred_element_type=jnp.float32)
    cos_real = result[:length, :width]
    cos_imag = result[:length, width:]
    sin_real = result[length:, :width]
    sin_imag = result[length:, width:]
    return (cos_real - sign * sin_imag, cos_imag + sign * sin_real)


def inverse(backward, real_part, imag_part, scale):
    count = backward.shape[0] // 2
    width = real_part.shape[1]
    joined = jnp.concatenate([real_part, imag_part], axis=1)
    result = jnp.dot(
        backward, joined, precision=lax.Precision.HIGH, preferred_element_type=jnp.float32
    )
    cos_real = result[:count, :width]
    cos_imag = result[:count, width:]
    sin_real = result[count:, :width]
    sin_imag = result[count:, width:]
    return ((cos_real - sin_imag) * scale, (cos_imag + sin_real) * scale)


def complex_mul(left, right):
    return (left[0] * right[0] - left[1] * right[1], left[0] * right[1] + left[1] * right[0])


def restack(real_part, imag_part, shape):
    return jnp.stack([real_part.reshape(shape), imag_part.reshape(shape)], axis=1).astype(
        jnp.bfloat16
    )


def batched(left, right):
    return jnp.einsum("eij,ejk->eik", left, right, preferred_element_type=jnp.float32)


def dyson(sigma_real, sigma_imag, g_free):
    free_real = g_free[:, 0]
    free_imag = g_free[:, 1]
    right_real = (batched(sigma_real, free_real) - batched(sigma_imag, free_imag)).astype(
        jnp.bfloat16
    )
    right_imag = (batched(sigma_real, free_imag) + batched(sigma_imag, free_real)).astype(
        jnp.bfloat16
    )
    out_real = (
        free_real.astype(jnp.float32)
        + batched(free_real, right_real)
        - batched(free_imag, right_imag)
    )
    out_imag = (
        free_imag.astype(jnp.float32)
        + batched(free_real, right_imag)
        + batched(free_imag, right_real)
    )
    return jnp.stack([out_real, out_imag], axis=1).astype(jnp.bfloat16)


def plain(g_lesser, g_greater, g_free, coulomb):
    length = 2 * NE
    upper, lower, backward = dft_tables(length, NE)
    tables = (upper, lower)
    scale = 1.0 / (length * NE)
    greater_t = jnp.swapaxes(g_greater, 2, 3)
    lesser_rows, greater_rows = (
        lax.all_to_all(g_lesser, "ea", split_axis=2, concat_axis=0, tiled=True),
        lax.all_to_all(greater_t, "ea", split_axis=2, concat_axis=0, tiled=True),
    )
    spec_lesser = forward(tables, lesser_rows, -1.0)
    element_shape = (NE, lesser_rows.shape[2], lesser_rows.shape[3])
    spec_greater = forward(tables, greater_rows, 1.0)
    joined = complex_mul(spec_lesser, spec_greater)
    polar_real, polar_imag = inverse(backward, joined[0], joined[1], scale)
    polar_rows = restack(polar_real, polar_imag, element_shape)
    polar = lax.all_to_all(polar_rows, "ea", split_axis=0, concat_axis=2, tiled=True)
    mixed_real = jnp.einsum(
        "eij,jk->eik", polar[:, 0], coulomb, preferred_element_type=jnp.float32
    ).astype(jnp.bfloat16)
    mixed_imag = jnp.einsum(
        "eij,jk->eik", polar[:, 1], coulomb, preferred_element_type=jnp.float32
    ).astype(jnp.bfloat16)
    square_real = batched(mixed_real, mixed_real) - batched(mixed_imag, mixed_imag)
    square_imag = batched(mixed_real, mixed_imag) + batched(mixed_imag, mixed_real)
    inner_real = (mixed_real.astype(jnp.float32) + square_real).astype(jnp.bfloat16)
    inner_imag = (mixed_imag.astype(jnp.float32) + square_imag).astype(jnp.bfloat16)
    screen_real = coulomb.astype(jnp.float32)[None] + jnp.einsum(
        "ij,ejk->eik", coulomb, inner_real, preferred_element_type=jnp.float32
    )
    screen_imag = jnp.einsum("ij,ejk->eik", coulomb, inner_imag, preferred_element_type=jnp.float32)
    screen = jnp.stack([screen_real, screen_imag], axis=1).astype(jnp.bfloat16)
    screen_rows = lax.all_to_all(screen, "ea", split_axis=2, concat_axis=0, tiled=True)
    spec_screen = forward(tables, screen_rows, -1.0)
    folded = complex_mul(spec_lesser, spec_screen)
    sigma_real, sigma_imag = inverse(backward, folded[0], folded[1], scale)
    sigma_rows = restack(sigma_real, sigma_imag, element_shape)
    sigma = lax.all_to_all(sigma_rows, "ea", split_axis=0, concat_axis=2, tiled=True)
    return dyson(sigma[:, 0], sigma[:, 1], g_free)


MESH = pl.DeviceIdType.MESH
CHUNKS = 4
VMEM_BYTES = 60 * 1024 * 1024


def transform_table(count):
    length = 2 * count
    phase = np.arange(length)[:, None] * np.arange(count)[None, :] % length
    angle = phase * (2.0 * math.pi / length)
    cosine, sine = np.cos(angle), np.sin(angle)
    return np.block([[cosine, sine], [-sine, cosine]]).astype(np.float32)


def greet(n):
    me = lax.axis_index("ea")
    barrier = pltpu.get_barrier_semaphore()

    def hello(k, carry):
        pl.semaphore_signal(
            barrier, inc=1, device_id={"ea": lax.rem(me + k, n)}, device_id_type=MESH
        )
        return carry

    lax.fori_loop(1, n, hello, 0)
    pl.semaphore_wait(barrier, n - 1)


def exchange_kernel(
    n, count, first, scale, *refs
):
    if first:
        (lesser, other, table, table_t, volts, out, kept,
         lesser_buf, other_buf, folded, in_send, in_recv, out_send, out_recv, own_in, own_out, keep) = refs
        streams = ((lesser, lesser_buf), (other, other_buf))
    else:
        (kept, other, table, table_t, out,
         lesser_buf, other_buf, folded, in_send, in_recv, out_send, out_recv, own_in, own_out, keep) = refs
        streams = ((other, other_buf),)
    me = lax.axis_index("ea")
    rows = folded.shape[1]
    each = count // n
    group = rows // CHUNKS

    def incoming(s, q, k):
        peer = lax.rem(me + k, n)
        source, target = streams[s]
        return pltpu.make_async_remote_copy(
            src_ref=source.at[:, pl.ds(peer * rows + q * group, group)],
            dst_ref=target.at[:, pl.ds(q * group, group), pl.ds(me * each, each)],
            send_sem=in_send.at[s, q, k],
            recv_sem=in_recv.at[s, q, k],
            device_id={"ea": peer},
            device_id_type=MESH,
        )

    def outgoing(q, k):
        peer = lax.rem(me + k, n)
        return pltpu.make_async_remote_copy(
            src_ref=folded.at[:, pl.ds(q * group, group), pl.ds(peer * each, each)],
            dst_ref=out.at[:, pl.ds(me * rows + q * group, group)],
            send_sem=out_send.at[q, k],
            recv_sem=out_recv.at[q, k],
            device_id={"ea": peer},
            device_id_type=MESH,
        )

    def own_incoming(s):
        source, target = streams[s]
        return pltpu.make_async_copy(
            source.at[:, pl.ds(me * rows, rows)],
            target.at[:, :, pl.ds(me * each, each)],
            own_in.at[s],
        )

    if not first:
        pltpu.make_async_copy(kept, lesser_buf, keep).start()
    for s in range(len(streams)):
        own_incoming(s).start()
    greet(n)

    def send_chunk(q, carry):
        for s in range(len(streams)):
            def send_one(k, inner):
                incoming(s, q, k).start()
                return inner
            lax.fori_loop(1, n, send_one, 0)
        return carry

    lax.fori_loop(0, CHUNKS, send_chunk, 0)
    for s in range(len(streams)):
        own_incoming(s).wait()
    if not first:
        pltpu.make_async_copy(kept, lesser_buf, keep).wait()

    length = 2 * count

    def fold(row, carry):
        left = jnp.concatenate([lesser_buf[0, row], lesser_buf[1, row]], axis=0)
        imag = other_buf[1, row]
        right = jnp.concatenate([other_buf[0, row], -imag if first else imag], axis=0)
        left_spec = jnp.dot(table[...], left, preferred_element_type=jnp.float32)
        right_spec = jnp.dot(table[...], right, preferred_element_type=jnp.float32)
        left_real, left_imag = left_spec[:length], left_spec[length:]
        right_real, right_imag = right_spec[:length], right_spec[length:]
        if first:
            real = left_real * right_real + left_imag * right_imag
            imag = left_imag * right_real - left_real * right_imag
        else:
            real = left_real * right_real - left_imag * right_imag
            imag = left_real * right_imag + left_imag * right_real
        product = jnp.concatenate([real, imag], axis=0).astype(jnp.bfloat16)
        result = jnp.dot(table_t[...], product, preferred_element_type=jnp.float32) * scale
        result = result.astype(jnp.bfloat16)
        if first:
            result = jnp.dot(result, volts[...], preferred_element_type=jnp.float32)
            result = result.astype(jnp.bfloat16)
        folded[0, row] = result[:count]
        folded[1, row] = result[count:]
        return carry

    def work(q, carry):
        for s in range(len(streams)):
            def wait_one(k, inner):
                incoming(s, q, k).wait()
                return inner
            lax.fori_loop(1, n, wait_one, 0)
        lax.fori_loop(q * group, (q + 1) * group, fold, 0)

        def send_one(k, inner):
            outgoing(q, k).start()
            return inner

        lax.fori_loop(1, n, send_one, 0)
        return carry

    lax.fori_loop(0, CHUNKS, work, 0)
    own_result = pltpu.make_async_copy(
        folded.at[:, :, pl.ds(me * each, each)], out.at[:, pl.ds(me * rows, rows)], own_out
    )
    own_result.start()
    if first:
        keeping = pltpu.make_async_copy(lesser_buf, kept, keep)
        keeping.start()

    def finish(q, carry):
        def wait_one(k, inner):
            outgoing(q, k).wait()
            return inner
        return lax.fori_loop(1, n, wait_one, carry)

    lax.fori_loop(0, CHUNKS, finish, 0)
    own_result.wait()
    if first:
        keeping.wait()


def exchange(n, count, first, scale, operands):
    two, orbitals, each, width = operands[1].shape
    rows = orbitals // n
    hbm = pl.BlockSpec(memory_space=pl.ANY)
    vmem = pl.BlockSpec(memory_space=pltpu.VMEM)
    streams = 2 if first else 1
    out_shape = [jax.ShapeDtypeStruct((2, orbitals, each, width), jnp.bfloat16)]
    if first:
        out_shape.append(jax.ShapeDtypeStruct((2, rows, count, width), jnp.bfloat16))
    buffer = pltpu.VMEM((2, rows, count, width), jnp.bfloat16)
    dma = pltpu.SemaphoreType.DMA
    return pl.pallas_call(
        functools.partial(exchange_kernel, n, count, first, scale),
        name="polarize" if first else "dress",
        out_shape=out_shape,
        in_specs=[hbm, hbm] + [vmem] * (len(operands) - 2),
        out_specs=[hbm] * len(out_shape),
        scratch_shapes=[
            buffer, buffer, buffer,
            dma((streams, CHUNKS, n)), dma((streams, CHUNKS, n)),
            dma((CHUNKS, n)), dma((CHUNKS, n)),
            dma((streams,)), dma, dma,
        ],
        compiler_params=pltpu.CompilerParams(
            collective_id=0 if first else 1, has_side_effects=True, vmem_limit_bytes=VMEM_BYTES
        ),
    )(*operands)


def dot(left, right):
    return jnp.dot(left, right, preferred_element_type=jnp.float32)


def screen_kernel(mixed, volts, out):
    bare = volts[...]
    for e in range(mixed.shape[0]):
        real, imag = mixed[e, 0], mixed[e, 1]
        square_real = dot(real, real) - dot(imag, imag)
        square_imag = dot(real, imag) + dot(imag, real)
        inner_real = (real.astype(jnp.float32) + square_real).astype(jnp.bfloat16)
        inner_imag = (imag.astype(jnp.float32) + square_imag).astype(jnp.bfloat16)
        out[e, 0] = (bare.astype(jnp.float32) + dot(bare, inner_real)).astype(jnp.bfloat16)
        out[e, 1] = dot(bare, inner_imag).astype(jnp.bfloat16)


def dyson_kernel(sigma, free, out):
    for e in range(sigma.shape[0]):
        real, imag = sigma[e, 0], sigma[e, 1]
        free_real, free_imag = free[e, 0], free[e, 1]
        right_real = (dot(real, free_real) - dot(imag, free_imag)).astype(jnp.bfloat16)
        right_imag = (dot(real, free_imag) + dot(imag, free_real)).astype(jnp.bfloat16)
        out_real = dot(free_real, right_real) - dot(free_imag, right_imag)
        out_imag = dot(free_real, right_imag) + dot(free_imag, right_real)
        out[e, 0] = (free_real.astype(jnp.float32) + out_real).astype(jnp.bfloat16)
        out[e, 1] = (free_imag.astype(jnp.float32) + out_imag).astype(jnp.bfloat16)


def per_energy(kernel, name, matrices, others):
    each, two, rows, width = matrices.shape
    block = pl.BlockSpec((2, two, rows, width), lambda i: (i, 0, 0, 0))
    specs = [block if other.ndim == 4 else pl.BlockSpec(memory_space=pltpu.VMEM) for other in others]
    products = 6 if name == "screen" else 8
    return pl.pallas_call(
        kernel,
        name=name,
        grid=(each // 2,),
        out_shape=jax.ShapeDtypeStruct(matrices.shape, jnp.bfloat16),
        in_specs=[block] + specs,
        out_specs=block,
        cost_estimate=pl.CostEstimate(
            flops=2 * products * each * rows * rows * width,
            bytes_accessed=4 * two * each * rows * width,
            transcendentals=0,
        ),
    )(matrices, *others)


def per_device(n, g_lesser, g_greater, g_free, coulomb):
    each, _, orbitals, _ = g_lesser.shape
    count = n * each
    if each % 16 or orbitals % (n * CHUNKS):
        return plain(g_lesser, g_greater, g_free, coulomb)
    scale = 1.0 / (2 * count * count)
    full = transform_table(count)
    table = jnp.asarray(full).astype(jnp.bfloat16)
    table_t = jnp.asarray(full.T).astype(jnp.bfloat16)
    lesser = jnp.transpose(g_lesser, (1, 2, 0, 3))
    greater = jnp.transpose(g_greater, (1, 3, 0, 2))
    mixed, kept = exchange(n, count, True, scale, (lesser, greater, table, table_t, coulomb))
    mixed = jnp.transpose(mixed, (2, 0, 1, 3))
    screen = per_energy(screen_kernel, "screen", mixed, (coulomb,))
    screen = jnp.transpose(screen, (1, 2, 0, 3))
    (sigma,) = exchange(n, count, False, scale, (kept, screen, table, table_t))
    sigma = jnp.transpose(sigma, (2, 0, 1, 3))
    return per_energy(dyson_kernel, "dyson", sigma, (g_free,))


def solution(mesh):
    return jax.shard_map(
        functools.partial(per_device, mesh.shape["ea"]),
        mesh=mesh,
        in_specs=(
            P(("bias", "ea"), None, None, None),
            P(("bias", "ea"), None, None, None),
            P(("bias", "ea"), None, None, None),
            P(),
        ),
        out_specs=P(("bias", "ea"), None, None, None),
        check_vma=False,
    )
```

```python
import functools
import math

import jax
import jax.numpy as jnp
import numpy as np
from jax import lax
from jax.experimental import pallas as pl
from jax.experimental.pallas import tpu as pltpu
from jax.sharding import PartitionSpec as P

NE = 256


def dft_tables(length, count):
    freq = jnp.arange(length, dtype=jnp.int32)
    places = jnp.arange(count, dtype=jnp.int32)
    phase = freq[:, None] * places[None, :] % length
    angle = phase.astype(jnp.float32) * (2.0 * math.pi / length)
    cosine = jnp.cos(angle)
    sine = jnp.sin(angle)
    stacked = jnp.concatenate([cosine, sine], axis=0)
    upper = stacked.astype(jnp.bfloat16)
    lower = (stacked - upper.astype(jnp.float32)).astype(jnp.bfloat16)
    backward = jnp.concatenate([cosine.T, sine.T], axis=0)
    return (upper, lower, backward)


def forward(tables, block, sign):
    upper, lower = tables
    length = upper.shape[0] // 2
    real_part = block[:, 0].reshape(block.shape[0], -1)
    imag_part = block[:, 1].reshape(block.shape[0], -1)
    width = real_part.shape[1]
    joined = jnp.concatenate([real_part, imag_part], axis=1)
    result = jnp.dot(upper, joined, preferred_element_type=jnp.float32)
    result = result + jnp.dot(lower, joined, preferred_element_type=jnp.float32)
    cos_real = result[:length, :width]
    cos_imag = result[:length, width:]
    sin_real = result[length:, :width]
    sin_imag = result[length:, width:]
    return (cos_real - sign * sin_imag, cos_imag + sign * sin_real)


def inverse(backward, real_part, imag_part, scale):
    count = backward.shape[0] // 2
    width = real_part.shape[1]
    joined = jnp.concatenate([real_part, imag_part], axis=1)
    result = jnp.dot(
        backward, joined, precision=lax.Precision.HIGH, preferred_element_type=jnp.float32
    )
    cos_real = result[:count, :width]
    cos_imag = result[:count, width:]
    sin_real = result[count:, :width]
    sin_imag = result[count:, width:]
    return ((cos_real - sin_imag) * scale, (cos_imag + sin_real) * scale)


def complex_mul(left, right):
    return (left[0] * right[0] - left[1] * right[1], left[0] * right[1] + left[1] * right[0])


def restack(real_part, imag_part, shape):
    return jnp.stack([real_part.reshape(shape), imag_part.reshape(shape)], axis=1).astype(
        jnp.bfloat16
    )


def batched(left, right):
    return jnp.einsum("eij,ejk->eik", left, right, preferred_element_type=jnp.float32)


def dyson(sigma_real, sigma_imag, g_free):
    free_real = g_free[:, 0]
    free_imag = g_free[:, 1]
    right_real = (batched(sigma_real, free_real) - batched(sigma_imag, free_imag)).astype(
        jnp.bfloat16
    )
    right_imag = (batched(sigma_real, free_imag) + batched(sigma_imag, free_real)).astype(
        jnp.bfloat16
    )
    out_real = (
        free_real.astype(jnp.float32)
        + batched(free_real, right_real)
        - batched(free_imag, right_imag)
    )
    out_imag = (
        free_imag.astype(jnp.float32)
        + batched(free_real, right_imag)
        + batched(free_imag, right_real)
    )
    return jnp.stack([out_real, out_imag], axis=1).astype(jnp.bfloat16)


def plain(g_lesser, g_greater, g_free, coulomb):
    length = 2 * NE
    upper, lower, backward = dft_tables(length, NE)
    tables = (upper, lower)
    scale = 1.0 / (length * NE)
    greater_t = jnp.swapaxes(g_greater, 2, 3)
    lesser_rows, greater_rows = (
        lax.all_to_all(g_lesser, "ea", split_axis=2, concat_axis=0, tiled=True),
        lax.all_to_all(greater_t, "ea", split_axis=2, concat_axis=0, tiled=True),
    )
    spec_lesser = forward(tables, lesser_rows, -1.0)
    element_shape = (NE, lesser_rows.shape[2], lesser_rows.shape[3])
    spec_greater = forward(tables, greater_rows, 1.0)
    joined = complex_mul(spec_lesser, spec_greater)
    polar_real, polar_imag = inverse(backward, joined[0], joined[1], scale)
    polar_rows = restack(polar_real, polar_imag, element_shape)
    polar = lax.all_to_all(polar_rows, "ea", split_axis=0, concat_axis=2, tiled=True)
    mixed_real = jnp.einsum(
        "eij,jk->eik", polar[:, 0], coulomb, preferred_element_type=jnp.float32
    ).astype(jnp.bfloat16)
    mixed_imag = jnp.einsum(
        "eij,jk->eik", polar[:, 1], coulomb, preferred_element_type=jnp.float32
    ).astype(jnp.bfloat16)
    square_real = batched(mixed_real, mixed_real) - batched(mixed_imag, mixed_imag)
    square_imag = batched(mixed_real, mixed_imag) + batched(mixed_imag, mixed_real)
    inner_real = (mixed_real.astype(jnp.float32) + square_real).astype(jnp.bfloat16)
    inner_imag = (mixed_imag.astype(jnp.float32) + square_imag).astype(jnp.bfloat16)
    screen_real = coulomb.astype(jnp.float32)[None] + jnp.einsum(
        "ij,ejk->eik", coulomb, inner_real, preferred_element_type=jnp.float32
    )
    screen_imag = jnp.einsum("ij,ejk->eik", coulomb, inner_imag, preferred_element_type=jnp.float32)
    screen = jnp.stack([screen_real, screen_imag], axis=1).astype(jnp.bfloat16)
    screen_rows = lax.all_to_all(screen, "ea", split_axis=2, concat_axis=0, tiled=True)
    spec_screen = forward(tables, screen_rows, -1.0)
    folded = complex_mul(spec_lesser, spec_screen)
    sigma_real, sigma_imag = inverse(backward, folded[0], folded[1], scale)
    sigma_rows = restack(sigma_real, sigma_imag, element_shape)
    sigma = lax.all_to_all(sigma_rows, "ea", split_axis=0, concat_axis=2, tiled=True)
    return dyson(sigma[:, 0], sigma[:, 1], g_free)


MESH = pl.DeviceIdType.MESH
CHUNKS = 4
LANES = 128
VMEM_BYTES = 60 * 1024 * 1024


def transform_table(count):
    length = 2 * count
    phase = np.arange(length)[:, None] * np.arange(count)[None, :] % length
    angle = phase * (2.0 * math.pi / length)
    cosine, sine = np.cos(angle), np.sin(angle)
    return np.block([[cosine, sine], [-sine, cosine]]).astype(np.float32)


def greet(n):
    me = lax.axis_index("ea")
    barrier = pltpu.get_barrier_semaphore()

    def hello(k, carry):
        pl.semaphore_signal(
            barrier, inc=1, device_id={"ea": lax.rem(me + k, n)}, device_id_type=MESH
        )
        return carry

    lax.fori_loop(1, n, hello, 0)
    pl.semaphore_wait(barrier, n - 1)


def exchange_kernel(
    n, count, first, scale, *refs
):
    if first:
        (lesser, other, table, table_t, volts, out, kept,
         lesser_buf, other_buf, folded, in_send, in_recv, out_send, out_recv, own_in, own_out, keep,
         lesser_raw, other_raw, lesser_rows, other_rows) = refs
        streams = ((lesser_rows, lesser_buf), (other_rows, other_buf))
    else:
        (kept, other, table, table_t, out,
         lesser_buf, other_buf, folded, in_send, in_recv, out_send, out_recv, own_in, own_out, keep) = refs
        streams = ((other, other_buf),)
    me = lax.axis_index("ea")
    rows = folded.shape[1]
    each = count // n
    group = rows // CHUNKS

    def incoming(s, q, k):
        peer = lax.rem(me + k, n)
        source, target = streams[s]
        return pltpu.make_async_remote_copy(
            src_ref=source.at[:, pl.ds(peer * rows + q * group, group)],
            dst_ref=target.at[:, pl.ds(q * group, group), pl.ds(me * each, each)],
            send_sem=in_send.at[s, q, k],
            recv_sem=in_recv.at[s, q, k],
            device_id={"ea": peer},
            device_id_type=MESH,
        )

    def outgoing(q, k):
        peer = lax.rem(me + k, n)
        return pltpu.make_async_remote_copy(
            src_ref=folded.at[:, pl.ds(q * group, group), pl.ds(peer * each, each)],
            dst_ref=out.at[:, pl.ds(me * rows + q * group, group)],
            send_sem=out_send.at[q, k],
            recv_sem=out_recv.at[q, k],
            device_id={"ea": peer},
            device_id_type=MESH,
        )

    def own_incoming(s):
        source, target = streams[s]
        return pltpu.make_async_copy(
            source.at[:, pl.ds(me * rows, rows)],
            target.at[:, :, pl.ds(me * each, each)],
            own_in.at[s],
        )

    def send_chunk(s, q):
        def send_one(k, inner):
            incoming(s, q, k).start()
            return inner

        lax.fori_loop(1, n, send_one, 0)

    if first:
        raw = (
            pltpu.make_async_copy(lesser, lesser_raw, own_in.at[0]),
            pltpu.make_async_copy(other, other_raw, own_in.at[1]),
        )
        for copy in raw:
            copy.start()
        greet(n)
        raw[0].wait()
        mine = pl.ds(pl.multiple_of(me * each, each), each)

        def regroup(k, carry):
            peer = lax.rem(me + k, n)
            block = pl.ds(pl.multiple_of(peer * rows, rows), rows)
            for c in range(2):
                lesser_rows[c, block] = jnp.swapaxes(lesser_raw[:, c, block, :], 0, 1)
            return carry

        def regroup_and_send(k, carry):
            regroup(k, carry)

            def send_one(q, inner):
                incoming(0, q, k).start()
                return inner

            return lax.fori_loop(0, CHUNKS, send_one, carry)

        lax.fori_loop(1, n, regroup_and_send, 0)
        regroup(0, 0)
        raw[1].wait()
        for low in range(0, rows * n, LANES):
            for c in range(2):
                turned = jnp.stack(
                    [other_raw[e, c, :, low : low + LANES].T for e in range(each)], axis=0
                )
                other_rows[c, low : low + LANES] = jnp.swapaxes(turned, 0, 1)
        lax.fori_loop(0, CHUNKS, lambda q, carry: (send_chunk(1, q), carry)[1], 0)
        for source, target in streams:
            for c in range(2):
                target[c, :, mine, :] = source[c, pl.ds(me * rows, rows)]
    else:
        pltpu.make_async_copy(kept, lesser_buf, keep).start()
        own_incoming(0).start()
        greet(n)
        lax.fori_loop(0, CHUNKS, lambda q, carry: (send_chunk(0, q), carry)[1], 0)
        own_incoming(0).wait()
        pltpu.make_async_copy(kept, lesser_buf, keep).wait()

    length = 2 * count

    def fold(row, carry):
        left = jnp.concatenate([lesser_buf[0, row], lesser_buf[1, row]], axis=0)
        imag = other_buf[1, row]
        right = jnp.concatenate([other_buf[0, row], -imag if first else imag], axis=0)
        left_spec = jnp.dot(table[...], left, preferred_element_type=jnp.float32)
        right_spec = jnp.dot(table[...], right, preferred_element_type=jnp.float32)
        left_real, left_imag = left_spec[:length], left_spec[length:]
        right_real, right_imag = right_spec[:length], right_spec[length:]
        if first:
            real = left_real * right_real + left_imag * right_imag
            imag = left_imag * right_real - left_real * right_imag
        else:
            real = left_real * right_real - left_imag * right_imag
            imag = left_real * right_imag + left_imag * right_real
        product = jnp.concatenate([real, imag], axis=0).astype(jnp.bfloat16)
        result = jnp.dot(table_t[...], product, preferred_element_type=jnp.float32) * scale
        result = result.astype(jnp.bfloat16)
        if first:
            result = jnp.dot(result, volts[...], preferred_element_type=jnp.float32)
            result = result.astype(jnp.bfloat16)
        folded[0, row] = result[:count]
        folded[1, row] = result[count:]
        return carry

    def work(q, carry):
        for s in range(len(streams)):
            def wait_one(k, inner):
                incoming(s, q, k).wait()
                return inner
            lax.fori_loop(1, n, wait_one, 0)
        lax.fori_loop(q * group, (q + 1) * group, fold, 0)

        def send_one(k, inner):
            outgoing(q, k).start()
            return inner

        lax.fori_loop(1, n, send_one, 0)
        return carry

    lax.fori_loop(0, CHUNKS, work, 0)
    own_result = pltpu.make_async_copy(
        folded.at[:, :, pl.ds(me * each, each)], out.at[:, pl.ds(me * rows, rows)], own_out
    )
    own_result.start()
    if first:
        keeping = pltpu.make_async_copy(lesser_buf, kept, keep)
        keeping.start()

    def finish(q, carry):
        def wait_one(k, inner):
            outgoing(q, k).wait()
            return inner
        return lax.fori_loop(1, n, wait_one, carry)

    lax.fori_loop(0, CHUNKS, finish, 0)
    own_result.wait()
    if first:
        keeping.wait()


def exchange(n, count, first, scale, operands):
    orbitals, width = operands[1].shape[-3 if not first else -2], operands[1].shape[-1]
    each = count // n
    rows = orbitals // n
    hbm = pl.BlockSpec(memory_space=pl.ANY)
    vmem = pl.BlockSpec(memory_space=pltpu.VMEM)
    streams = 2 if first else 1
    out_shape = [jax.ShapeDtypeStruct((2, orbitals, each, width), jnp.bfloat16)]
    if first:
        out_shape.append(jax.ShapeDtypeStruct((2, rows, count, width), jnp.bfloat16))
    buffer = pltpu.VMEM((2, rows, count, width), jnp.bfloat16)
    dma = pltpu.SemaphoreType.DMA
    staging = []
    if first:
        staging = [pltpu.VMEM((each, 2, orbitals, width), jnp.bfloat16)] * 2
        staging += [pltpu.VMEM((2, orbitals, each, width), jnp.bfloat16)] * 2
    return pl.pallas_call(
        functools.partial(exchange_kernel, n, count, first, scale),
        name="polarize" if first else "dress",
        out_shape=out_shape,
        in_specs=[hbm, hbm] + [vmem] * (len(operands) - 2),
        out_specs=[hbm] * len(out_shape),
        scratch_shapes=[
            buffer, buffer, buffer,
            dma((streams, CHUNKS, n)), dma((streams, CHUNKS, n)),
            dma((CHUNKS, n)), dma((CHUNKS, n)),
            dma((streams,)), dma, dma,
        ] + staging,
        compiler_params=pltpu.CompilerParams(
            collective_id=0 if first else 1, has_side_effects=True, vmem_limit_bytes=VMEM_BYTES
        ),
    )(*operands)


def dot(left, right):
    return jnp.dot(left, right, preferred_element_type=jnp.float32)


def screen_kernel(mixed, volts, out):
    bare = volts[...]
    for e in range(mixed.shape[0]):
        real, imag = mixed[e, 0], mixed[e, 1]
        square_real = dot(real, real) - dot(imag, imag)
        square_imag = dot(real, imag) + dot(imag, real)
        inner_real = (real.astype(jnp.float32) + square_real).astype(jnp.bfloat16)
        inner_imag = (imag.astype(jnp.float32) + square_imag).astype(jnp.bfloat16)
        out[e, 0] = (bare.astype(jnp.float32) + dot(bare, inner_real)).astype(jnp.bfloat16)
        out[e, 1] = dot(bare, inner_imag).astype(jnp.bfloat16)


def dyson_kernel(sigma, free, out):
    for e in range(sigma.shape[0]):
        real, imag = sigma[e, 0], sigma[e, 1]
        free_real, free_imag = free[e, 0], free[e, 1]
        right_real = (dot(real, free_real) - dot(imag, free_imag)).astype(jnp.bfloat16)
        right_imag = (dot(real, free_imag) + dot(imag, free_real)).astype(jnp.bfloat16)
        out_real = dot(free_real, right_real) - dot(free_imag, right_imag)
        out_imag = dot(free_real, right_imag) + dot(free_imag, right_real)
        out[e, 0] = (free_real.astype(jnp.float32) + out_real).astype(jnp.bfloat16)
        out[e, 1] = (free_imag.astype(jnp.float32) + out_imag).astype(jnp.bfloat16)


def per_energy(kernel, name, matrices, others):
    each, two, rows, width = matrices.shape
    block = pl.BlockSpec((2, two, rows, width), lambda i: (i, 0, 0, 0))
    specs = [block if other.ndim == 4 else pl.BlockSpec(memory_space=pltpu.VMEM) for other in others]
    products = 6 if name == "screen" else 8
    return pl.pallas_call(
        kernel,
        name=name,
        grid=(each // 2,),
        out_shape=jax.ShapeDtypeStruct(matrices.shape, jnp.bfloat16),
        in_specs=[block] + specs,
        out_specs=block,
        cost_estimate=pl.CostEstimate(
            flops=2 * products * each * rows * rows * width,
            bytes_accessed=4 * two * each * rows * width,
            transcendentals=0,
        ),
    )(matrices, *others)


def per_device(n, g_lesser, g_greater, g_free, coulomb):
    each, _, orbitals, _ = g_lesser.shape
    count = n * each
    if each % 16 or orbitals % (n * 16) or orbitals % LANES:
        return plain(g_lesser, g_greater, g_free, coulomb)
    scale = 1.0 / (2 * count * count)
    full = transform_table(count)
    table = jnp.asarray(full).astype(jnp.bfloat16)
    table_t = jnp.asarray(full.T).astype(jnp.bfloat16)
    mixed, kept = exchange(n, count, True, scale, (g_lesser, g_greater, table, table_t, coulomb))
    mixed = jnp.transpose(mixed, (2, 0, 1, 3))
    screen = per_energy(screen_kernel, "screen", mixed, (coulomb,))
    screen = jnp.transpose(screen, (1, 2, 0, 3))
    (sigma,) = exchange(n, count, False, scale, (kept, screen, table, table_t))
    sigma = jnp.transpose(sigma, (2, 0, 1, 3))
    return per_energy(dyson_kernel, "dyson", sigma, (g_free,))


def solution(mesh):
    return jax.shard_map(
        functools.partial(per_device, mesh.shape["ea"]),
        mesh=mesh,
        in_specs=(
            P(("bias", "ea"), None, None, None),
            P(("bias", "ea"), None, None, None),
            P(("bias", "ea"), None, None, None),
            P(),
        ),
        out_specs=P(("bias", "ea"), None, None, None),
        check_vma=False,
    )
```
